32 devices in a mesh: dp: 1 (over z), sp: 32 (over y, x, core).
Axes of the slice: x: 4, y: 4, z: 1, core: 2. Of those that a mesh axis runs over, the one named last changes fastest.
The devices are a block of a 4x4x8 slice.
Arguments:
- tokens: bfloat16 [128, 4096], P('dp')
- w_query: bfloat16 [4096, 4096], replicated
- w_key: bfloat16 [4096, 128], replicated
- w_value: bfloat16 [4096, 128], replicated
- w_out: bfloat16 [4096, 4096], P('sp')
- k_cache: bfloat16 [128, 8192, 128], P('dp', 'sp')
- v_cache: bfloat16 [128, 8192, 128], P('dp', 'sp')
- positions: int32 [128], P('dp')
Outputs:
- output 1: bfloat16 [128, 4096], P('dp')
- output 2: bfloat16 [128, 8192, 128], P('dp', 'sp')
- output 3: bfloat16 [128, 8192, 128], P('dp', 'sp')
All inputs are finite; a program needn't handle non-finite values.
Results may differ from the reference program's by a relative error of at most 0.00420465.
Values are sent between devices in bfloat16 or wider.
A program may use at most 768 MiB of HBM per device.

```python
import jax
import jax.numpy as jnp
import math
from jax import lax

BATCH_ROWS = 128
SEQ_LEN = 8192
D_MODEL = 4096
N_HEADS = 32
HEAD_DIM = 128
GAIN_BLOCK = 32


def setup_inputs(seed: int = 0, part: int = 0) -> dict:
    root = jax.random.key(seed)
    shared = jax.random.split(root, 4)
    local = jax.random.split(jax.random.fold_in(root, part), 5)
    q_width = N_HEADS * HEAD_DIM
    align_scale = (math.log(SEQ_LEN) + 0.5) * HEAD_DIM ** -0.5
    tokens = jax.random.normal(local[0], (BATCH_ROWS, D_MODEL), jnp.float32)
    key_raw = jax.random.normal(shared[1], (D_MODEL, HEAD_DIM), jnp.float32)
    w_query = (jax.random.normal(shared[0], (D_MODEL, q_width), jnp.float32) + align_scale * jnp.tile(key_raw, (1, N_HEADS))) * D_MODEL ** -0.5
    w_key = key_raw * D_MODEL ** -0.5
    w_value = jax.random.normal(shared[2], (D_MODEL, HEAD_DIM), jnp.float32) * D_MODEL ** -0.5
    w_out = jax.random.normal(shared[3], (q_width, D_MODEL), jnp.float32) * q_width ** -0.5
    n_blocks = SEQ_LEN // GAIN_BLOCK
    key_gains = jax.random.uniform(local[1], (BATCH_ROWS, n_blocks, 1, 1), jnp.float32, 0.6, 1.6)
    k_cache = (jax.random.normal(local[2], (BATCH_ROWS, n_blocks, GAIN_BLOCK, HEAD_DIM), jnp.float32) * key_gains).reshape(BATCH_ROWS, SEQ_LEN, HEAD_DIM)
    v_cache = jax.random.normal(local[3], (BATCH_ROWS, SEQ_LEN, HEAD_DIM), jnp.float32)
    positions = jax.random.randint(local[4], (BATCH_ROWS,), SEQ_LEN // 4, SEQ_LEN, jnp.int32)
    positions = positions.at[0].set(SEQ_LEN - 1).at[1].set(SEQ_LEN // 4)
    return dict(tokens=tokens.astype(jnp.bfloat16), w_query=w_query.astype(jnp.bfloat16), w_key=w_key.astype(jnp.bfloat16), w_value=w_value.astype(jnp.bfloat16), w_out=w_out.astype(jnp.bfloat16), k_cache=k_cache.astype(jnp.bfloat16), v_cache=v_cache.astype(jnp.bfloat16), positions=positions)


def reference(tokens, w_query, w_key, w_value, w_out, k_cache, v_cache, positions):
    queries = jnp.dot(tokens, w_query, preferred_element_type=jnp.float32).astype(jnp.bfloat16)
    queries = queries.reshape(BATCH_ROWS, N_HEADS, HEAD_DIM)
    key_new = jnp.dot(tokens, w_key, preferred_element_type=jnp.float32).astype(jnp.bfloat16)
    value_new = jnp.dot(tokens, w_value, preferred_element_type=jnp.float32).astype(jnp.bfloat16)
    slot_ids = jnp.arange(SEQ_LEN)
    hit_mask = (slot_ids[None, :] == positions[:, None])[:, :, None]
    k_upd = jnp.where(hit_mask, key_new[:, None, :], k_cache)
    v_upd = jnp.where(hit_mask, value_new[:, None, :], v_cache)

    def one_row(row_args):
        q_row, k_row, v_row, pos_row = row_args
        scores = jnp.dot(q_row, k_row.T, preferred_element_type=jnp.float32) * HEAD_DIM ** -0.5
        scores = jnp.where(slot_ids[None, :] <= pos_row, scores, -jnp.inf)
        weights = jnp.exp(scores - jnp.max(scores, axis=1, keepdims=True))
        weight_sum = jnp.sum(weights, axis=1)
        value_sum = jnp.dot(weights.astype(jnp.bfloat16), v_row, preferred_element_type=jnp.float32)
        return value_sum / weight_sum[:, None]

    head_outs = lax.map(one_row, (queries, k_upd, v_upd, positions))
    attn_heads = head_outs.astype(jnp.bfloat16).reshape(BATCH_ROWS, N_HEADS * HEAD_DIM)
    attn_out = jnp.dot(attn_heads, w_out, preferred_element_type=jnp.float32).astype(jnp.bfloat16)
    return (attn_out, k_upd, v_upd)
```

```python
import functools
import math

import jax
import jax.numpy as jnp
from jax import lax
from jax.experimental import pallas as pl
from jax.experimental.pallas import tpu as pltpu
from jax.sharding import PartitionSpec as P

MESH = pl.DeviceIdType.MESH
BF16, F32 = jnp.bfloat16, jnp.float32
LOWEST = -3.0e38


class Grid:
    def __init__(self, n):
        self.n = n
        self.a = a = math.isqrt(n // 2)
        me = lax.axis_index('sp')
        self.me = me
        self.c = lax.rem(me, 2)
        self.x = lax.rem(me // 2, a)
        self.y = me // (2 * a)

    def index(self, y, x, c):
        return (y * self.a + x) * 2 + c

    def y_at(self, r):
        return lax.rem(self.y + r, self.a)

    def x_at(self, r):
        return lax.rem(self.x + r, self.a)

    def y_peer(self, r):
        return self.index(self.y_at(r), self.x, self.c)

    def x_peer(self, r):
        return self.index(self.y, self.x_at(r), self.c)

    def partner(self):
        return self.index(self.y, self.x, 1 - self.c)

    def peers(self):
        out = [self.partner()]
        for r in range(1, self.a):
            out += [self.y_peer(r), self.x_peer(r)]
        return out

    def greet(self):
        barrier = pltpu.get_barrier_semaphore()
        for p in self.peers():
            pl.semaphore_signal(barrier, inc=1, device_id={'sp': p}, device_id_type=MESH)

    def greeted(self):
        pl.semaphore_wait(pltpu.get_barrier_semaphore(), 2 * self.a - 1)


def remote(src, dst, send, recv, dev):
    return pltpu.make_async_remote_copy(src_ref=src, dst_ref=dst, send_sem=send, recv_sem=recv, device_id={'sp': dev}, device_id_type=MESH)


class Gather:
    def __init__(self, g, buf, send, recv):
        self.g, self.buf, self.send, self.recv = g, buf, send, recv
        rows = buf.shape[3]
        self.lo, self.hi = pl.ds(0, rows // 2), pl.ds(rows // 2, rows // 2)

    def ring_copies(self, first):
        g, buf, a = self.g, self.buf, self.g.a
        out = []
        for r in range(1, a):
            if first:
                srcs = (buf.at[g.y, g.x, g.c, self.lo], buf.at[g.y, g.x, g.c, self.hi])
            else:
                srcs = (buf.at[:, g.x, g.c, self.lo], buf.at[g.y, :, g.c, self.hi])
            peers = (g.y_peer(r), g.x_peer(r)) if first else (g.x_peer(r), g.y_peer(r))
            for i in range(2):
                k = ((0 if first else 2) + i) * (a - 1) + r - 1
                out.append(remote(srcs[i], srcs[i], self.send.at[k], self.recv.at[k], peers[i]))
        return out

    def start(self):
        self.first = self.ring_copies(True)
        for cp in self.first:
            cp.start()

    def finish(self):
        g, buf = self.g, self.buf
        for cp in self.first:
            cp.wait_recv()
        second = self.ring_copies(False)
        for cp in second:
            cp.start()
        for cp in second:
            cp.wait_recv()
        k = 4 * (g.a - 1)
        plane = buf.at[:, :, g.c]
        last = remote(plane, plane, self.send.at[k], self.recv.at[k], g.partner())
        last.start()
        last.wait_recv()
        for cp in self.first + second + [last]:
            cp.wait_send()

    @staticmethod
    def sems(a):
        return 4 * (a - 1) + 1


def project_kernel(n, x_hbm, wq_hbm, wk_hbm, wv_hbm, q_out, kv_out, xv, wqv, wkv, lsem, send, recv):
    g = Grid(n)
    hd = wqv.shape[1]
    col = pl.multiple_of(g.me * hd, hd)
    copies = [
        pltpu.make_async_copy(x_hbm, xv, lsem.at[0]),
        pltpu.make_async_copy(wq_hbm.at[:, pl.ds(col, hd)], wqv, lsem.at[1]),
        pltpu.make_async_copy(wk_hbm, wkv.at[:, pl.ds(0, hd)], lsem.at[2]),
        pltpu.make_async_copy(wv_hbm, wkv.at[:, pl.ds(hd, hd)], lsem.at[3]),
    ]
    for cp in copies:
        cp.start()
    g.greet()
    copies[0].wait()
    copies[1].wait()
    q = jnp.dot(xv[...], wqv[...], preferred_element_type=F32).astype(BF16)
    q_out[g.y, g.x, g.c] = q
    g.greeted()
    gather = Gather(g, q_out, send, recv)
    gather.start()
    copies[2].wait()
    copies[3].wait()
    kv = jnp.dot(xv[...], wkv[...], preferred_element_type=F32).astype(BF16)
    kv_out[0] = kv[:, :hd].astype(F32)
    kv_out[1] = kv[:, hd:].astype(F32)
    gather.finish()


def attend_kernel(blk, pos, q_ref, kv_new, k_hbm, v_hbm, ko_hbm, vo_hbm, o_ref, ml_ref, kbuf, vbuf, q32, rsem, wsem):
    n_rows, t_loc, hd = kbuf.shape
    n_heads = o_ref.shape[0] // n_rows
    n_blk = n_rows // blk
    base = lax.axis_index('sp') * t_loc
    scale = hd ** -0.5 * math.log2(math.e)

    def reads(i):
        rows = pl.ds(i * blk, blk)
        return (pltpu.make_async_copy(k_hbm.at[rows], kbuf.at[rows], rsem.at[0, i]), pltpu.make_async_copy(v_hbm.at[rows], vbuf.at[rows], rsem.at[1, i]))

    def writes(i):
        rows = pl.ds(i * blk, blk)
        return (pltpu.make_async_copy(kbuf.at[rows], ko_hbm.at[rows], wsem.at[0, i]), pltpu.make_async_copy(vbuf.at[rows], vo_hbm.at[rows], wsem.at[1, i]))

    @pl.loop(0, n_blk)
    def _(i):
        for cp in reads(i):
            cp.start()

    @pl.loop(0, n_heads)
    def _(h):
        q32[pl.ds(h * n_rows, n_rows), :] = q_ref[h].astype(F32)

    ml_ref[...] = jnp.zeros_like(ml_ref)
    lane = lax.broadcasted_iota(jnp.int32, (n_heads, t_loc), 1)
    lane_b = lax.broadcasted_iota(jnp.int32, (n_heads, n_rows), 1)
    tile_row = lax.broadcasted_iota(jnp.int32, (16, hd), 0)

    @pl.loop(0, n_blk)
    def _(i):
        for cp in reads(i):
            cp.wait()
        slots = []
        for u in range(blk):
            b = i * blk + u
            p = pos[b] - base
            slots.append((b, p))
            t0 = pl.multiple_of(jnp.clip(p, 0, t_loc - 1) // 16 * 16, 16)
            hit = tile_row == p - t0
            for which, buf in enumerate((kbuf, vbuf)):
                new = jnp.broadcast_to(kv_new[which, pl.ds(b, 1), :], (16, hd))
                old = buf[b, pl.ds(t0, 16), :].astype(F32)
                buf[b, pl.ds(t0, 16), :] = jnp.where(hit, new, old).astype(BF16)
        for cp in writes(i):
            cp.start()
        m_acc, l_acc = ml_ref[0], ml_ref[1]
        for b, p in slots:
            qb = q32[pl.ds(b, n_heads, stride=n_rows), :].astype(BF16)
            s = lax.dot_general(qb, kbuf[b], (((1,), (1,)), ((), ())), preferred_element_type=F32) * scale
            s = jnp.where(lane <= p, s, -jnp.inf)
            m = jnp.maximum(jnp.max(s, axis=1, keepdims=True), LOWEST)
            w = jnp.exp2(s - m)
            l = jnp.sum(w, axis=1, keepdims=True)
            o = jnp.dot(w.astype(BF16), vbuf[b], preferred_element_type=F32)
            o_ref[pl.ds(b, n_heads, stride=n_rows), :] = o
            m_acc = jnp.where(lane_b == b, m, m_acc)
            l_acc = jnp.where(lane_b == b, l, l_acc)
        ml_ref[0] = m_acc
        ml_ref[1] = l_acc

    @pl.loop(0, n_blk)
    def _(i):
        for cp in writes(i):
            cp.wait()


def merge(ms, ls):
    top = functools.reduce(jnp.maximum, ms)
    fs = [jnp.exp2(m - top) for m in ms]
    total = functools.reduce(jnp.add, [l * f for l, f in zip(ls, fs)])
    return top, fs, total


def combine_kernel(n, o_ref, ml_ref, wo_ref, y_out, r0, ml0, rows, fa, fb, fcol, mla, mlb, r1a, r1b, rmla, rmlb, s2a, s2b, sm2a, sm2b, r2a, r2b, rm2a, rm2b, go, send0, recv0, send1, recv1, send2, recv2, asend, arecv, bsend, brecv):
    g = Grid(n)
    a = g.a
    n_rows, hd = o_ref.shape[3:]
    half = n_rows // 2
    lo, hi = pl.ds(0, half), pl.ds(half, half)
    g.greet()
    g.greeted()
    order = sorted(range(a - 1), key=lambda r: -min(r + 1, a - 1 - r)) + [a - 1]

    ml_cp = remote(ml_ref, ml0, send0.at[2 * a], recv0.at[2 * a], g.partner())
    ml_cp.start()
    core_a, core_b = {}, {}
    for r in order:
        hy, hx = g.y_at(r + 1), g.x_at(r + 1)
        core_a[r] = remote(o_ref.at[hy, :, 1 - g.c, lo], r0.at[hy, :, lo], send0.at[r], recv0.at[r], g.partner())
        core_b[r] = remote(o_ref.at[:, hx, 1 - g.c, hi], r0.at[:, hx, hi], send0.at[a + r], recv0.at[a + r], g.partner())
        core_a[r].start()
        core_b[r].start()
    ml_cp.wait_recv()
    own = pl.ds(g.c, a * a, stride=2)
    top, fs, total = merge([ml_ref[0, own, :], ml0[0, own, :]], [ml_ref[1, own, :], ml0[1, own, :]])
    for i, v in enumerate([top, total] + fs):
        rows[i] = v
    for i in range(a):
        for k, (da, db) in enumerate(((mla, mlb), (mla, mlb), (fa, fb), (fa, fb))):
            dst = pl.ds(k % 2 * a, a)
            da[i, dst, :] = rows[k, pl.ds(i * a, a), :]
            db[i, dst, :] = rows[k, pl.ds(i, a, stride=a), :]

    ring1 = []
    for r in order:
        hy, hx = g.y_at(r + 1), g.x_at(r + 1)
        core_a[r].wait_recv()
        ft = fa[hy].T[:half]
        for j in range(a):
            r0[hy, j, lo] = o_ref[hy, j, g.c, lo] * ft[:, j:j + 1] + r0[hy, j, lo] * ft[:, a + j:a + j + 1]
        if r < a - 1:
            ring1 += [
                remote(mla.at[hy], rmla.at[r], send1.at[0, r], recv1.at[0, r], g.y_peer(r + 1)),
                remote(r0.at[hy, :, lo], r1a.at[r], send1.at[1, r], recv1.at[1, r], g.y_peer(r + 1)),
            ]
            ring1[-2].start()
            ring1[-1].start()
        core_b[r].wait_recv()
        ft = fb[hx].T[half:]
        for j in range(a):
            r0[j, hx, hi] = o_ref[j, hx, g.c, hi] * ft[:, j:j + 1] + r0[j, hx, hi] * ft[:, a + j:a + j + 1]
        if r < a - 1:
            ring1 += [
                remote(mlb.at[hx], rmlb.at[r], send1.at[2, r], recv1.at[2, r], g.x_peer(r + 1)),
                remote(r0.at[:, hx, hi], r1b.at[r], send1.at[3, r], recv1.at[3, r], g.x_peer(r + 1)),
            ]
            ring1[-2].start()
            ring1[-1].start()
    for cp in ring1:
        cp.wait_recv()

    for side, (ml_own, ml_got, dst, sm) in enumerate(((mla, rmla, s2a, sm2a), (mlb, rmlb, s2b, sm2b))):
        place = g.x if side else g.y
        parts = [ml_own.at[place]] + [ml_got.at[r] for r in range(a - 1)]
        top, fs, total = merge([p[pl.ds(0, a), :] for p in parts], [p[pl.ds(a, a), :] for p in parts])
        for s in range(a):
            fcol[pl.ds(s * a, a), :] = fs[s]
        rows[0, pl.ds(0, a), :] = top
        rows[1, pl.ds(0, a), :] = total
        ft = fcol[...].T[half * side:half * (side + 1)]
        for j in range(a):
            sm[j, 0:1, :] = rows[0, j:j + 1, :]
            sm[j, 1:2, :] = rows[1, j:j + 1, :]
            acc = (r0[j, g.x, hi] if side else r0[g.y, j, lo]) * ft[:, j:j + 1]
            for r in range(a - 1):
                got = r1b[r, j] if side else r1a[r, j]
                acc = acc + got * ft[:, (r + 1) * a + j:(r + 1) * a + j + 1]
            dst[j] = acc

    ring2 = []
    for r in order[:-1]:
        hy, hx = g.y_at(r + 1), g.x_at(r + 1)
        ring2 += [
            remote(sm2a.at[hx], rm2a.at[r], send2.at[0, r], recv2.at[0, r], g.x_peer(r + 1)),
            remote(s2a.at[hx], r2a.at[r], send2.at[1, r], recv2.at[1, r], g.x_peer(r + 1)),
            remote(sm2b.at[hy], rm2b.at[r], send2.at[2, r], recv2.at[2, r], g.y_peer(r + 1)),
            remote(s2b.at[hy], r2b.at[r], send2.at[3, r], recv2.at[3, r], g.y_peer(r + 1)),
        ]
    for cp in ring2:
        cp.start()
    for cp in ring2:
        cp.wait_recv()
    for side, (sm, rm, mine, got) in enumerate(((sm2a, rm2a, s2a, r2a), (sm2b, rm2b, s2b, r2b))):
        place = g.y if side else g.x
        parts = [sm.at[place]] + [rm.at[r] for r in range(a - 1)]
        top, fs, total = merge([p[0:1, :] for p in parts], [p[1:2, :] for p in parts])
        for s in range(a):
            fcol[pl.ds(s, 1), :] = fs[s]
        fcol[pl.ds(a, 1), :] = total
        ft = fcol[...].T[half * side:half * (side + 1)]
        acc = mine[place] * ft[:, 0:1]
        for r in range(a - 1):
            acc = acc + got[r] * ft[:, r + 1:r + 2]
        go[g.y, g.x, g.c, (hi if side else lo), :] = (acc / ft[:, a:a + 1]).astype(BF16)

    heads = Gather(g, go, asend, arecv)
    heads.start()
    heads.finish()
    acc = jnp.zeros((n_rows, wo_ref.shape[1]), F32)
    for k in range(a * a):
        lhs = jnp.concatenate([go[k // a, k % a, 0], go[k // a, k % a, 1]], axis=1)
        acc = acc + jnp.dot(lhs, wo_ref[pl.ds(k * 2 * hd, 2 * hd), :], preferred_element_type=F32)
    y_out[g.y, g.x, g.c] = acc.astype(BF16)
    outs = Gather(g, y_out, bsend, brecv)
    outs.start()
    outs.finish()
    for cp in [ml_cp] + list(core_a.values()) + list(core_b.values()) + ring1 + ring2:
        cp.wait_send()


def solution(mesh):
    n = mesh.shape['sp']
    a = math.isqrt(n // 2)
    vmem, hbm, smem = (pl.BlockSpec(memory_space=s) for s in (pltpu.VMEM, pltpu.HBM, pltpu.SMEM))
    dma = pltpu.SemaphoreType.DMA

    def local_step(tokens, w_query, w_key, w_value, w_out, k_cache, v_cache, positions):
        n_rows, t_loc, hd = k_cache.shape
        d_model = tokens.shape[1]
        wo = lax.all_to_all(w_out.reshape(w_out.shape[0], n, -1), 'sp', split_axis=1, concat_axis=0, tiled=True)
        wo = wo.reshape(w_out.shape[0] * n, -1)
        half = n_rows // 2
        sems = [dma((Gather.sems(a),))] * 2
        q_all, kv_new = pl.pallas_call(
            functools.partial(project_kernel, n),
            out_shape=(jax.ShapeDtypeStruct((a, a, 2, n_rows, hd), BF16), jax.ShapeDtypeStruct((2, n_rows, hd), F32)),
            in_specs=[hbm] * 4,
            out_specs=(vmem, vmem),
            scratch_shapes=[pltpu.VMEM((n_rows, d_model), BF16), pltpu.VMEM((d_model, hd), BF16), pltpu.VMEM((d_model, 2 * hd), BF16), dma((4,))] + sems,
            compiler_params=pltpu.CompilerParams(collective_id=0, has_side_effects=True, vmem_limit_bytes=10 << 20),
            name='project',
        )(tokens, w_query, w_key, w_value)
        blk = 8
        cache = jax.ShapeDtypeStruct(k_cache.shape, k_cache.dtype)
        k_upd, v_upd, o, ml = pl.pallas_call(
            functools.partial(attend_kernel, blk),
            out_shape=(cache, cache, jax.ShapeDtypeStruct((n * n_rows, hd), F32), jax.ShapeDtypeStruct((2, n, n_rows), F32)),
            in_specs=[smem, vmem, vmem, hbm, hbm],
            out_specs=(hbm, hbm, vmem, vmem),
            scratch_shapes=[pltpu.VMEM(k_cache.shape, BF16)] * 2 + [pltpu.VMEM((n * n_rows, hd), F32)] + [dma((2, n_rows // blk))] * 2,
            compiler_params=pltpu.CompilerParams(vmem_limit_bytes=28 << 20),
            name='attend',
        )(positions, q_all.reshape(n, n_rows, hd), kv_new, k_cache, v_cache)
        f32 = lambda *s: pltpu.VMEM(s, F32)
        y = pl.pallas_call(
            functools.partial(combine_kernel, n),
            out_shape=jax.ShapeDtypeStruct((a, a, 2, n_rows, w_out.shape[1] // n), BF16),
            in_specs=[vmem] * 3,
            out_specs=vmem,
            scratch_shapes=[f32(a, a, n_rows, hd), f32(2, n, n_rows), f32(4, a * a, n_rows)]
            + [f32(a, 2 * a, n_rows)] * 2 + [f32(max(a * a, 8), n_rows)] + [f32(a, 2 * a, n_rows)] * 2
            + [f32(a - 1, a, half, hd)] * 2 + [f32(a - 1, 2 * a, n_rows)] * 2
            + [f32(a, half, hd)] * 2 + [f32(a, 8, n_rows)] * 2 + [f32(a - 1, half, hd)] * 2 + [f32(a - 1, 8, n_rows)] * 2
            + [pltpu.VMEM((a, a, 2, n_rows, hd), BF16)]
            + [dma((2 * a + 1,))] * 2 + [dma((4, a - 1))] * 4 + sems * 2,
            compiler_params=pltpu.CompilerParams(collective_id=1, has_side_effects=True, vmem_limit_bytes=14 << 20),
            name='combine',
        )(o.reshape(a, a, 2, n_rows, hd), ml, wo)
        y = y.reshape(n, n_rows, -1).transpose(1, 0, 2).reshape(n_rows, -1)
        return y, k_upd, v_upd

    cache_spec = P('dp', 'sp', None)
    return jax.shard_map(local_step, mesh=mesh, in_specs=(P('dp', None), P(), P(), P(), P('sp', None), cache_spec, cache_spec, P('dp')), out_specs=(P('dp', None), cache_spec, cache_spec), check_vma=False)
```

```python
import functools
import math

import jax
import jax.numpy as jnp
from jax import lax
from jax.experimental import pallas as pl
from jax.experimental.pallas import tpu as pltpu
from jax.sharding import PartitionSpec as P

MESH = pl.DeviceIdType.MESH
BF16, F32 = jnp.bfloat16, jnp.float32
LOWEST = -3.0e38


class Grid:
    def __init__(self, n):
        self.n = n
        self.a = a = math.isqrt(n // 2)
        me = lax.axis_index('sp')
        self.me = me
        self.c = lax.rem(me, 2)
        self.x = lax.rem(me // 2, a)
        self.y = me // (2 * a)

    def index(self, y, x, c):
        return (y * self.a + x) * 2 + c

    def y_at(self, r):
        return lax.rem(self.y + r, self.a)

    def x_at(self, r):
        return lax.rem(self.x + r, self.a)

    def y_peer(self, r):
        return self.index(self.y_at(r), self.x, self.c)

    def x_peer(self, r):
        return self.index(self.y, self.x_at(r), self.c)

    def partner(self):
        return self.index(self.y, self.x, 1 - self.c)

    def peers(self):
        out = [self.partner()]
        for r in range(1, self.a):
            out += [self.y_peer(r), self.x_peer(r)]
        return out

    def greet(self):
        barrier = pltpu.get_barrier_semaphore()
        for p in self.peers():
            pl.semaphore_signal(barrier, inc=1, device_id={'sp': p}, device_id_type=MESH)

    def greeted(self):
        pl.semaphore_wait(pltpu.get_barrier_semaphore(), 2 * self.a - 1)


def remote(src, dst, send, recv, dev):
    return pltpu.make_async_remote_copy(src_ref=src, dst_ref=dst, send_sem=send, recv_sem=recv, device_id={'sp': dev}, device_id_type=MESH)


class Gather:
    def __init__(self, g, buf, send, recv):
        self.g, self.buf, self.send, self.recv = g, buf, send, recv
        rows = buf.shape[3]
        self.lo, self.hi = pl.ds(0, rows // 2), pl.ds(rows // 2, rows // 2)

    def ring_copies(self, first):
        g, buf, a = self.g, self.buf, self.g.a
        out = []
        for r in range(1, a):
            if first:
                srcs = (buf.at[g.c, g.y, g.x, self.lo], buf.at[g.c, g.y, g.x, self.hi])
            else:
                srcs = (buf.at[g.c, :, g.x, self.lo], buf.at[g.c, g.y, :, self.hi])
            peers = (g.y_peer(r), g.x_peer(r)) if first else (g.x_peer(r), g.y_peer(r))
            for i in range(2):
                k = ((0 if first else 2) + i) * (a - 1) + r - 1
                out.append(remote(srcs[i], srcs[i], self.send.at[k], self.recv.at[k], peers[i]))
        return out

    def start(self):
        self.first = self.ring_copies(True)
        for cp in self.first:
            cp.start()

    def finish(self):
        g, buf = self.g, self.buf
        for cp in self.first:
            cp.wait_recv()
        second = self.ring_copies(False)
        for cp in second:
            cp.start()
        for cp in second:
            cp.wait_recv()
        k = 4 * (g.a - 1)
        plane = buf.at[g.c]
        last = remote(plane, plane, self.send.at[k], self.recv.at[k], g.partner())
        last.start()
        last.wait_recv()
        for cp in self.first + second + [last]:
            cp.wait_send()

    @staticmethod
    def sems(a):
        return 4 * (a - 1) + 1


def project_kernel(n, x_hbm, wq_hbm, wk_hbm, wv_hbm, wo_hbm, q_out, kv_out, wo_out, xv, wqv, wkv, lsem, wsem, send, recv):
    g = Grid(n)
    hd = wqv.shape[1]
    col = pl.multiple_of(g.me * hd, hd)
    copies = [
        pltpu.make_async_copy(x_hbm, xv, lsem.at[0]),
        pltpu.make_async_copy(wq_hbm.at[:, pl.ds(col, hd)], wqv, lsem.at[1]),
        pltpu.make_async_copy(wk_hbm, wkv.at[:, pl.ds(0, hd)], lsem.at[2]),
        pltpu.make_async_copy(wv_hbm, wkv.at[:, pl.ds(hd, hd)], lsem.at[3]),
    ]
    rows, width = wo_hbm.shape[0], wo_hbm.shape[1] // 2
    mine = wo_out.at[pl.ds(pl.multiple_of(g.c * rows, rows), rows)]
    copies.append(pltpu.make_async_copy(wo_hbm.at[:, pl.ds(pl.multiple_of(g.c * width, width), width)], mine, lsem.at[4]))
    for cp in copies:
        cp.start()
    g.greet()
    copies[0].wait()
    copies[1].wait()
    q = jnp.dot(xv[...], wqv[...], preferred_element_type=F32).astype(BF16)
    q_out[g.c, g.y, g.x] = q
    g.greeted()
    gather = Gather(g, q_out, send, recv)
    gather.start()
    swap = remote(wo_hbm.at[:, pl.ds(pl.multiple_of((1 - g.c) * width, width), width)], mine, wsem.at[0], wsem.at[1], g.partner())
    swap.start()
    copies[2].wait()
    copies[3].wait()
    kv = jnp.dot(xv[...], wkv[...], preferred_element_type=F32).astype(BF16)
    kv_out[0] = kv[:, :hd].astype(F32)
    kv_out[1] = kv[:, hd:].astype(F32)
    gather.finish()
    copies[4].wait()
    swap.wait()


def attend_kernel(blk, pos, q_ref, kv_new, k_hbm, v_hbm, ko_hbm, vo_hbm, o_ref, ml_ref, kbuf, vbuf, q32, s_s, w_s, rsem, wsem):
    n_rows, t_loc, hd = kbuf.shape
    n_heads = o_ref.shape[0] // n_rows
    n_blk = n_rows // blk
    base = lax.axis_index('sp') * t_loc
    scale = hd ** -0.5 * math.log2(math.e)

    def reads(i):
        rows = pl.ds(i * blk, blk)
        return (pltpu.make_async_copy(k_hbm.at[rows], kbuf.at[rows], rsem.at[0, i]), pltpu.make_async_copy(v_hbm.at[rows], vbuf.at[rows], rsem.at[1, i]))

    def writes(i):
        rows = pl.ds(i * blk, blk)
        return (pltpu.make_async_copy(kbuf.at[rows], ko_hbm.at[rows], wsem.at[0, i]), pltpu.make_async_copy(vbuf.at[rows], vo_hbm.at[rows], wsem.at[1, i]))

    @pl.loop(0, n_blk)
    def _(i):
        for cp in reads(i):
            cp.start()

    @pl.loop(0, n_heads)
    def _(h):
        q32[pl.ds(h * n_rows, n_rows), :] = q_ref[h].astype(F32)

    ml_ref[...] = jnp.zeros_like(ml_ref)
    lane = lax.broadcasted_iota(jnp.int32, (n_heads, t_loc), 1)
    lane_b = lax.broadcasted_iota(jnp.int32, (n_heads, n_rows), 1)
    tile_row = lax.broadcasted_iota(jnp.int32, (16, hd), 0)

    def intake(i):
        for cp in reads(i):
            cp.wait()
        stores = []
        for u in range(blk):
            b = i * blk + u
            p = pos[b] - base
            t0 = pl.multiple_of(jnp.clip(p, 0, t_loc - 1) // 16 * 16, 16)
            hit = tile_row == p - t0
            for which, buf in enumerate((kbuf, vbuf)):
                new = jnp.broadcast_to(kv_new[which, pl.ds(b, 1), :], (16, hd))
                old = buf[b, pl.ds(t0, 16), :].astype(F32)
                stores.append((buf, b, t0, jnp.where(hit, new, old).astype(BF16)))
        for buf, b, t0, v in stores:
            buf[b, pl.ds(t0, 16), :] = v
        for cp in writes(i):
            cp.start()

    def step(i, qk, soft, pv):
        outs, scores = [], []
        if pv:
            for u in range(blk):
                b = (i - 2) * blk + u
                outs.append((b, jnp.dot(w_s[u], vbuf[b], preferred_element_type=F32)))
        if soft:
            m_acc, l_acc = ml_ref[0], ml_ref[1]
            ss = [s_s[u] for u in range(blk)]
        if qk:
            for u in range(blk):
                b = i * blk + u
                qb = q32[pl.ds(b, n_heads, stride=n_rows), :].astype(BF16)
                scores.append(lax.dot_general(qb, kbuf[b], (((1,), (1,)), ((), ())), preferred_element_type=F32))
        if soft:
            for u, s in enumerate(ss):
                b = (i - 1) * blk + u
                s = jnp.where(lane <= pos[b] - base, s * scale, -jnp.inf)
                m = jnp.maximum(jnp.max(s, axis=1, keepdims=True), LOWEST)
                w = jnp.exp2(s - m)
                l = jnp.sum(w, axis=1, keepdims=True)
                w_s[u] = w.astype(BF16)
                m_acc = jnp.where(lane_b == b, m, m_acc)
                l_acc = jnp.where(lane_b == b, l, l_acc)
            ml_ref[0] = m_acc
            ml_ref[1] = l_acc
        for u, s in enumerate(scores):
            s_s[u] = s
        for b, o in outs:
            o_ref[pl.ds(b, n_heads, stride=n_rows), :] = o

    intake(0)
    step(0, True, False, False)
    intake(1)
    step(1, True, True, False)

    @pl.loop(2, n_blk)
    def _(i):
        intake(i)
        step(i, True, True, True)

    step(n_blk, False, True, True)
    step(n_blk + 1, False, False, True)

    @pl.loop(0, n_blk)
    def _(i):
        for cp in writes(i):
            cp.wait()


def merge(ms, ls):
    top = functools.reduce(jnp.maximum, ms)
    fs = [jnp.exp2(m - top) for m in ms]
    total = functools.reduce(jnp.add, [l * f for l, f in zip(ls, fs)])
    return top, fs, total


def combine_kernel(n, o_ref, ml_ref, wo_ref, y_out, r0, ml0, rows, fa, fb, fcol, mla, mlb, r1a, r1b, rmla, rmlb, s2a, s2b, sm2a, sm2b, r2a, r2b, rm2a, rm2b, go, r0y, y1a, y1b, t2a, t2b, y2a, y2b, send0, recv0, send1, recv1, send2, recv2, osem, send3, recv3, send4, recv4, bsend, brecv):
    g = Grid(n)
    a = g.a
    n_rows, hd = o_ref.shape[3:]
    half = n_rows // 2
    lo, hi = pl.ds(0, half), pl.ds(half, half)
    g.greet()
    g.greeted()
    order = sorted(range(a - 1), key=lambda r: -min(r + 1, a - 1 - r)) + [a - 1]

    ml_cp = remote(ml_ref, ml0, send0.at[2 * a], recv0.at[2 * a], g.partner())
    ml_cp.start()
    core_a, core_b = {}, {}
    for r in order:
        hy, hx = g.y_at(r + 1), g.x_at(r + 1)
        core_a[r] = remote(o_ref.at[1 - g.c, hy, :, lo], r0.at[hy, :, lo], send0.at[r], recv0.at[r], g.partner())
        core_b[r] = remote(o_ref.at[1 - g.c, :, hx, hi], r0.at[:, hx, hi], send0.at[a + r], recv0.at[a + r], g.partner())
        core_a[r].start()
        core_b[r].start()
    ml_cp.wait_recv()
    own = pl.ds(pl.multiple_of(g.c * a * a, a * a), a * a)
    top, fs, total = merge([ml_ref[0, own, :], ml0[0, own, :]], [ml_ref[1, own, :], ml0[1, own, :]])
    for i, v in enumerate([top, total] + fs):
        rows[i] = v
    for i in range(a):
        for k, (da, db) in enumerate(((mla, mlb), (mla, mlb), (fa, fb), (fa, fb))):
            dst = pl.ds(k % 2 * a, a)
            da[i, dst, :] = rows[k, pl.ds(i * a, a), :]
            db[i, dst, :] = rows[k, pl.ds(i, a, stride=a), :]

    ring1 = []
    for r in order:
        hy, hx = g.y_at(r + 1), g.x_at(r + 1)
        core_a[r].wait_recv()
        ft = fa[hy].T[:half]
        for j in range(a):
            r0[hy, j, lo] = o_ref[g.c, hy, j, lo] * ft[:, j:j + 1] + r0[hy, j, lo] * ft[:, a + j:a + j + 1]
        if r < a - 1:
            ring1 += [
                remote(mla.at[hy], rmla.at[r], send1.at[0, r], recv1.at[0, r], g.y_peer(r + 1)),
                remote(r0.at[hy, :, lo], r1a.at[r], send1.at[1, r], recv1.at[1, r], g.y_peer(r + 1)),
            ]
            ring1[-2].start()
            ring1[-1].start()
        core_b[r].wait_recv()
        ft = fb[hx].T[half:]
        for j in range(a):
            r0[j, hx, hi] = o_ref[g.c, j, hx, hi] * ft[:, j:j + 1] + r0[j, hx, hi] * ft[:, a + j:a + j + 1]
        if r < a - 1:
            ring1 += [
                remote(mlb.at[hx], rmlb.at[r], send1.at[2, r], recv1.at[2, r], g.x_peer(r + 1)),
                remote(r0.at[:, hx, hi], r1b.at[r], send1.at[3, r], recv1.at[3, r], g.x_peer(r + 1)),
            ]
            ring1[-2].start()
            ring1[-1].start()
    for cp in ring1:
        cp.wait_recv()

    for side, (ml_own, ml_got, dst, sm) in enumerate(((mla, rmla, s2a, sm2a), (mlb, rmlb, s2b, sm2b))):
        place = g.x if side else g.y
        parts = [ml_own.at[place]] + [ml_got.at[r] for r in range(a - 1)]
        top, fs, total = merge([p[pl.ds(0, a), :] for p in parts], [p[pl.ds(a, a), :] for p in parts])
        for s in range(a):
            fcol[pl.ds(s * a, a), :] = fs[s]
        rows[0, pl.ds(0, a), :] = top
        rows[1, pl.ds(0, a), :] = total
        ft = fcol[...].T[half * side:half * (side + 1)]
        for j in range(a):
            sm[j, 0:1, :] = rows[0, j:j + 1, :]
            sm[j, 1:2, :] = rows[1, j:j + 1, :]
            acc = (r0[j, g.x, hi] if side else r0[g.y, j, lo]) * ft[:, j:j + 1]
            for r in range(a - 1):
                got = r1b[r, j] if side else r1a[r, j]
                acc = acc + got * ft[:, (r + 1) * a + j:(r + 1) * a + j + 1]
            dst[j] = acc

    ring2 = []
    for r in order[:-1]:
        hy, hx = g.y_at(r + 1), g.x_at(r + 1)
        ring2 += [
            remote(sm2a.at[hx], rm2a.at[r], send2.at[0, r], recv2.at[0, r], g.x_peer(r + 1)),
            remote(s2a.at[hx], r2a.at[r], send2.at[1, r], recv2.at[1, r], g.x_peer(r + 1)),
            remote(sm2b.at[hy], rm2b.at[r], send2.at[2, r], recv2.at[2, r], g.y_peer(r + 1)),
            remote(s2b.at[hy], r2b.at[r], send2.at[3, r], recv2.at[3, r], g.y_peer(r + 1)),
        ]
    for cp in ring2:
        cp.start()
    for cp in ring2:
        cp.wait_recv()
    for side, (sm, rm, mine, got) in enumerate(((sm2a, rm2a, s2a, r2a), (sm2b, rm2b, s2b, r2b))):
        place = g.y if side else g.x
        parts = [sm.at[place]] + [rm.at[r] for r in range(a - 1)]
        top, fs, total = merge([p[0:1, :] for p in parts], [p[1:2, :] for p in parts])
        for s in range(a):
            fcol[pl.ds(s, 1), :] = fs[s]
        fcol[pl.ds(a, 1), :] = total
        ft = fcol[...].T[half * side:half * (side + 1)]
        acc = mine[place] * ft[:, 0:1]
        for r in range(a - 1):
            acc = acc + got[r] * ft[:, r + 1:r + 2]
        go[g.c, (hi if side else lo), :] = (acc / ft[:, a:a + 1]).astype(BF16)

    heads = remote(go.at[g.c], go.at[g.c], osem.at[0], osem.at[1], g.partner())
    heads.start()
    heads.wait_recv()
    lhs = jnp.concatenate([go[0], go[1]], axis=1)
    for i in range(a):
        part = jnp.dot(lhs, wo_ref[:, pl.ds(i * a * hd, a * hd)], preferred_element_type=F32)
        for j in range(a):
            r0y[i, j] = part[:, j * hd:(j + 1) * hd]
    ring3, ring4 = [], []
    for r in order[:-1]:
        hy, hx = g.y_at(r + 1), g.x_at(r + 1)
        ring3 += [
            remote(r0y.at[hy, :, lo], y1a.at[r], send3.at[0, r], recv3.at[0, r], g.y_peer(r + 1)),
            remote(r0y.at[:, hx, hi], y1b.at[r], send3.at[1, r], recv3.at[1, r], g.x_peer(r + 1)),
        ]
    for cp in ring3:
        cp.start()
    for cp in ring3:
        cp.wait_recv()
    t2a[...] = functools.reduce(jnp.add, [y1a[r] for r in range(a - 1)], r0y[g.y, :, lo])
    t2b[...] = functools.reduce(jnp.add, [y1b[r] for r in range(a - 1)], r0y[:, g.x, hi])
    for r in order[:-1]:
        hy, hx = g.y_at(r + 1), g.x_at(r + 1)
        ring4 += [
            remote(t2a.at[hx], y2a.at[r], send4.at[0, r], recv4.at[0, r], g.x_peer(r + 1)),
            remote(t2b.at[hy], y2b.at[r], send4.at[1, r], recv4.at[1, r], g.y_peer(r + 1)),
        ]
    for cp in ring4:
        cp.start()
    for cp in ring4:
        cp.wait_recv()
    y_out[g.c, g.y, g.x, lo, :] = functools.reduce(jnp.add, [y2a[r] for r in range(a - 1)], t2a[g.x]).astype(BF16)
    y_out[g.c, g.y, g.x, hi, :] = functools.reduce(jnp.add, [y2b[r] for r in range(a - 1)], t2b[g.y]).astype(BF16)
    outs = Gather(g, y_out, bsend, brecv)
    outs.start()
    outs.finish()
    for cp in [ml_cp, heads] + list(core_a.values()) + list(core_b.values()) + ring1 + ring2 + ring3 + ring4:
        cp.wait_send()


def solution(mesh):
    n = mesh.shape['sp']
    a = math.isqrt(n // 2)
    vmem, hbm, smem = (pl.BlockSpec(memory_space=s) for s in (pltpu.VMEM, pltpu.HBM, pltpu.SMEM))
    dma = pltpu.SemaphoreType.DMA

    def stay(x):
        return pltpu.with_memory_space_constraint(x, pltpu.HBM)

    def local_step(tokens, w_query, w_key, w_value, w_out, k_cache, v_cache, positions):
        n_rows, t_loc, hd = k_cache.shape
        d_model = tokens.shape[1]
        half = n_rows // 2
        f32 = lambda *s: pltpu.VMEM(s, F32)
        bf16 = lambda *s: pltpu.VMEM(s, BF16)
        shape = jax.ShapeDtypeStruct
        sems = [dma((Gather.sems(a),))] * 2
        q_all, kv_new, wo = pl.pallas_call(
            functools.partial(project_kernel, n),
            out_shape=(shape((2, a, a, n_rows, hd), BF16), shape((2, n_rows, hd), F32), shape((2 * w_out.shape[0], w_out.shape[1] // 2), BF16)),
            in_specs=[hbm] * 5,
            out_specs=(vmem,) * 3,
            scratch_shapes=[bf16(n_rows, d_model), bf16(d_model, hd), bf16(d_model, 2 * hd), dma((5,)), dma((2,))] + sems,
            compiler_params=pltpu.CompilerParams(collective_id=0, has_side_effects=True, vmem_limit_bytes=12 << 20),
            name='project',
        )(*map(stay, (tokens, w_query, w_key, w_value, w_out)))
        blk = 8
        cache = shape(k_cache.shape, k_cache.dtype)
        k_upd, v_upd, o, ml = pl.pallas_call(
            functools.partial(attend_kernel, blk),
            out_shape=(cache, cache, shape((n * n_rows, hd), F32), shape((2, n, n_rows), F32)),
            in_specs=[smem, vmem, vmem, hbm, hbm],
            out_specs=(hbm, hbm, vmem, vmem),
            scratch_shapes=[bf16(*k_cache.shape)] * 2 + [f32(n * n_rows, hd), f32(blk, n, t_loc), bf16(blk, n, t_loc)] + [dma((2, n_rows // blk))] * 2,
            compiler_params=pltpu.CompilerParams(vmem_limit_bytes=28 << 20),
            name='attend',
        )(positions, q_all.reshape(n, n_rows, hd), kv_new, stay(k_cache), stay(v_cache))
        y = pl.pallas_call(
            functools.partial(combine_kernel, n),
            out_shape=shape((2, a, a, n_rows, w_out.shape[1] // n), BF16),
            in_specs=[vmem] * 3,
            out_specs=vmem,
            scratch_shapes=[f32(a, a, n_rows, hd), f32(2, n, n_rows), f32(4, a * a, n_rows)]
            + [f32(a, 2 * a, n_rows)] * 2 + [f32(max(a * a, 8), n_rows)] + [f32(a, 2 * a, n_rows)] * 2
            + [f32(a - 1, a, half, hd)] * 2 + [f32(a - 1, 2 * a, n_rows)] * 2
            + [f32(a, half, hd)] * 2 + [f32(a, 8, n_rows)] * 2 + [f32(a - 1, half, hd)] * 2 + [f32(a - 1, 8, n_rows)] * 2
            + [bf16(2, n_rows, hd), f32(a, a, n_rows, hd)] + [f32(a - 1, a, half, hd)] * 2 + [f32(a, half, hd)] * 2 + [f32(a - 1, half, hd)] * 2
            + [dma((2 * a + 1,))] * 2 + [dma((4, a - 1))] * 4 + [dma((2,))] + [dma((2, a - 1))] * 4 + sems,
            compiler_params=pltpu.CompilerParams(collective_id=1, has_side_effects=True, vmem_limit_bytes=16 << 20),
            name='combine',
        )(o.reshape(2, a, a, n_rows, hd), ml, wo)
        y = y.reshape(n, n_rows, -1).transpose(1, 0, 2).reshape(n_rows, -1)
        return y, k_upd, v_upd

    cache_spec = P('dp', 'sp', None)
    return jax.shard_map(local_step, mesh=mesh, in_specs=(P('dp', None), P(), P(), P(), P('sp', None), cache_spec, cache_spec, P('dp')), out_specs=(P('dp', None), cache_spec, cache_spec), check_vma=False)
```

```python
import functools
import math

import jax
import jax.numpy as jnp
from jax import lax
from jax.experimental import pallas as pl
from jax.experimental.pallas import tpu as pltpu
from jax.sharding import PartitionSpec as P

MESH = pl.DeviceIdType.MESH
BF16, F32 = jnp.bfloat16, jnp.float32
LOWEST = -3.0e38


class Grid:
    def __init__(self, n):
        self.n = n
        self.a = a = math.isqrt(n // 2)
        me = lax.axis_index('sp')
        self.me = me
        self.c = lax.rem(me, 2)
        self.x = lax.rem(me // 2, a)
        self.y = me // (2 * a)

    def index(self, y, x, c):
        return (y * self.a + x) * 2 + c

    def y_at(self, r):
        return lax.rem(self.y + r, self.a)

    def x_at(self, r):
        return lax.rem(self.x + r, self.a)

    def y_peer(self, r):
        return self.index(self.y_at(r), self.x, self.c)

    def x_peer(self, r):
        return self.index(self.y, self.x_at(r), self.c)

    def partner(self):
        return self.index(self.y, self.x, 1 - self.c)

    def peers(self):
        out = [self.partner()]
        for r in range(1, self.a):
            out += [self.y_peer(r), self.x_peer(r)]
        return out

    def greet(self):
        barrier = pltpu.get_barrier_semaphore()
        for p in self.peers():
            pl.semaphore_signal(barrier, inc=1, device_id={'sp': p}, device_id_type=MESH)

    def greeted(self):
        pl.semaphore_wait(pltpu.get_barrier_semaphore(), 2 * self.a - 1)


def remote(src, dst, send, recv, dev):
    return pltpu.make_async_remote_copy(src_ref=src, dst_ref=dst, send_sem=send, recv_sem=recv, device_id={'sp': dev}, device_id_type=MESH)


class Gather:
    def __init__(self, g, buf, send, recv):
        self.g, self.buf, self.send, self.recv = g, buf, send, recv
        rows = buf.shape[3]
        self.half = (pl.ds(0, rows // 2), pl.ds(rows // 2, rows // 2))
        self.order = sorted(range(1, g.a), key=lambda r: -min(r, g.a - r))
        self.k = 0

    def cp(self, ref, dev):
        c = remote(ref, ref, self.send.at[self.k], self.recv.at[self.k], dev)
        self.k += 1
        c.start()
        return c

    def start(self):
        g, buf = self.g, self.buf
        self.first, self.late = {}, []
        for r in self.order:
            self.first[0, r] = self.cp(buf.at[g.c, g.y, g.x, self.half[0]], g.y_peer(r))
            self.first[1, r] = self.cp(buf.at[g.c, g.y, g.x, self.half[1]], g.x_peer(r))
        for r in self.order:
            self.late.append(((0, 0, r), self.cp(buf.at[g.c, g.y, g.x, self.half[0]], g.x_peer(r))))
            self.late.append(((1, 0, r), self.cp(buf.at[g.c, g.y, g.x, self.half[1]], g.y_peer(r))))
        self.core = [self.cp(buf.at[g.c, g.y, g.x], g.partner())]

    def finish(self):
        g, buf, a = self.g, self.buf, self.g.a
        for r in self.order[::-1]:
            for s in range(2):
                self.first[s, r].wait_recv()
                src = buf.at[g.c, g.y_at(a - r), g.x, self.half[0]] if s == 0 else buf.at[g.c, g.y, g.x_at(a - r), self.half[1]]
                for q in self.order:
                    self.late.append(((s, r, q), self.cp(src, g.x_peer(q) if s == 0 else g.y_peer(q))))
                self.core.append(self.cp(src, g.partner()))
        for (s, r, q), c in self.late:
            c.wait_recv()
            if s == 0:
                src = buf.at[g.c, g.y_at((a - r) % a), g.x_at(a - q), self.half[0]]
            else:
                src = buf.at[g.c, g.y_at(a - q), g.x_at((a - r) % a), self.half[1]]
            self.core.append(self.cp(src, g.partner()))
        for c in self.core:
            c.wait_recv()
        for c in list(self.first.values()) + [c for _, c in self.late] + self.core:
            c.wait_send()

    @staticmethod
    def sems(a):
        return 4 * (a - 1) + 1 + 2 * (a - 1) * a + 2 * (a - 1) * a


def project_kernel(n, x_hbm, wq_hbm, wk_hbm, wv_hbm, wo_hbm, k_hbm, v_hbm, q_out, kv_out, wo_out, k_out, v_out, xv, wqv, wkv, lsem, qsem, csem, rsem):
    g = Grid(n)
    hd = kv_out.shape[2]
    width = wq_hbm.shape[1] // 2
    n_part, part = wqv.shape[0], wqv.shape[2]
    x_cp = pltpu.make_async_copy(x_hbm, xv, lsem.at[0])
    q_cps = [
        pltpu.make_async_copy(wq_hbm.at[:, pl.ds(pl.multiple_of(g.c * width + i * part, part), part)], wqv.at[i], qsem.at[i])
        for i in range(n_part)
    ]
    kv_cps = [
        pltpu.make_async_copy(wk_hbm, wkv.at[:, pl.ds(0, hd)], lsem.at[1]),
        pltpu.make_async_copy(wv_hbm, wkv.at[:, pl.ds(hd, hd)], lsem.at[2]),
    ]
    rows, half = wo_hbm.shape[0], wo_hbm.shape[1] // 2
    mine = wo_out.at[pl.ds(pl.multiple_of(g.c * rows, rows), rows)]
    wo_cp = pltpu.make_async_copy(wo_hbm.at[:, pl.ds(pl.multiple_of(g.c * half, half), half)], mine, lsem.at[3])
    wo_swap = remote(wo_hbm.at[:, pl.ds(pl.multiple_of((1 - g.c) * half, half), half)], mine, rsem.at[0], rsem.at[1], g.partner())
    cache_cps = [pltpu.make_async_copy(k_hbm, k_out, csem.at[0]), pltpu.make_async_copy(v_hbm, v_out, csem.at[1])]
    x_cp.start()
    for cp in q_cps + kv_cps:
        cp.start()
    barrier = pltpu.get_barrier_semaphore()
    pl.semaphore_signal(barrier, inc=1, device_id={'sp': g.partner()}, device_id_type=MESH)
    x_cp.wait()
    per = part // hd
    first = g.c * (n // 4)
    for i in range(n_part):
        q_cps[i].wait()
        if i == n_part - 2:
            cache_cps[0].start()
        q = jnp.dot(xv[...], wqv[i], preferred_element_type=F32).astype(BF16)
        for j in range(i * per, (i + 1) * per):
            q_out[j % 2, first + j // 2] = q[:, (j - i * per) * hd:(j - i * per + 1) * hd]
    cache_cps[1].start()
    pl.semaphore_wait(barrier, 1)
    heads = q_out.at[:, pl.ds(first, n // 4)]
    q_swap = remote(heads, heads, rsem.at[2], rsem.at[3], g.partner())
    q_swap.start()
    wo_swap.start()
    wo_cp.start()
    for cp in kv_cps:
        cp.wait()
    kv = jnp.dot(xv[...], wkv[...], preferred_element_type=F32).astype(BF16)
    kv_out[0] = kv[:, :hd].astype(F32)
    kv_out[1] = kv[:, hd:].astype(F32)
    q_swap.wait()
    wo_swap.wait()
    for cp in [wo_cp] + cache_cps:
        cp.wait()


def attend_kernel(blk, pos, q_ref, kv_new, k_in, v_in, ko_hbm, vo_hbm, o_ref, ml_ref, kbuf, vbuf, q32, s_s, w_s, wsem):
    n_rows, t_loc, hd = kbuf.shape
    n_heads = o_ref.shape[0] // n_rows
    n_blk = n_rows // blk
    base = lax.axis_index('sp') * t_loc
    scale = hd ** -0.5 * math.log2(math.e)

    def writes(i):
        rows = pl.ds(i * blk, blk)
        return (pltpu.make_async_copy(kbuf.at[rows], ko_hbm.at[rows], wsem.at[0, i]), pltpu.make_async_copy(vbuf.at[rows], vo_hbm.at[rows], wsem.at[1, i]))

    @pl.loop(0, n_heads)
    def _(h):
        q32[pl.ds(h * n_rows, n_rows), :] = q_ref[h].astype(F32)

    ml_ref[...] = jnp.zeros_like(ml_ref)
    lane = lax.broadcasted_iota(jnp.int32, (n_heads, t_loc), 1)
    lane_b = lax.broadcasted_iota(jnp.int32, (n_heads, n_rows), 1)
    tile_row = lax.broadcasted_iota(jnp.int32, (16, hd), 0)

    def intake(i):
        stores = []
        for u in range(blk):
            b = i * blk + u
            p = pos[b] - base
            t0 = pl.multiple_of(jnp.clip(p, 0, t_loc - 1) // 16 * 16, 16)
            hit = tile_row == p - t0
            for which, buf in enumerate((kbuf, vbuf)):
                new = jnp.broadcast_to(kv_new[which, pl.ds(b, 1), :], (16, hd))
                old = buf[b, pl.ds(t0, 16), :].astype(F32)
                stores.append((buf, b, t0, jnp.where(hit, new, old).astype(BF16)))
        for buf, b, t0, v in stores:
            buf[b, pl.ds(t0, 16), :] = v
        for cp in writes(i):
            cp.start()

    def step(i, qk, soft, pv):
        outs, scores = [], []
        if pv:
            for u in range(blk):
                b = (i - 2) * blk + u
                outs.append((b, jnp.dot(w_s[u], vbuf[b], preferred_element_type=F32)))
        if soft:
            m_acc, l_acc = ml_ref[0], ml_ref[1]
            ss = [s_s[u] for u in range(blk)]
        if qk:
            for u in range(blk):
                b = i * blk + u
                qb = q32[pl.ds(b, n_heads, stride=n_rows), :].astype(BF16)
                scores.append(lax.dot_general(qb, kbuf[b], (((1,), (1,)), ((), ())), preferred_element_type=F32))
        if soft:
            for u, s in enumerate(ss):
                b = (i - 1) * blk + u
                s = jnp.where(lane <= pos[b] - base, s * scale, -jnp.inf)
                m = jnp.maximum(jnp.max(s, axis=1, keepdims=True), LOWEST)
                w = jnp.exp2(s - m)
                l = jnp.sum(w, axis=1, keepdims=True)
                w_s[u] = w.astype(BF16)
                m_acc = jnp.where(lane_b == b, m, m_acc)
                l_acc = jnp.where(lane_b == b, l, l_acc)
            ml_ref[0] = m_acc
            ml_ref[1] = l_acc
        for u, s in enumerate(scores):
            s_s[u] = s
        for b, o in outs:
            o_ref[pl.ds(b, n_heads, stride=n_rows), :] = o

    intake(0)
    step(0, True, False, False)
    intake(1)
    step(1, True, True, False)

    @pl.loop(2, n_blk)
    def _(i):
        intake(i)
        step(i, True, True, True)

    step(n_blk, False, True, True)
    step(n_blk + 1, False, False, True)

    @pl.loop(0, n_blk)
    def _(i):
        for cp in writes(i):
            cp.wait()


def merge(ms, ls):
    top = functools.reduce(jnp.maximum, ms)
    fs = [jnp.exp2(m - top) for m in ms]
    total = functools.reduce(jnp.add, [l * f for l, f in zip(ls, fs)])
    return top, fs, total


def combine_kernel(n, o_ref, ml_ref, wo_ref, y_out, r0, ml0, rows, fa, fb, fcol, mla, mlb, r1a, r1b, rmla, rmlb, s2a, s2b, sm2a, sm2b, r2a, r2b, rm2a, rm2b, go, r0y, y1a, y1b, t2a, t2b, y2a, y2b, send0, recv0, send1, recv1, send2, recv2, osem, send3, recv3, send4, recv4, bsend, brecv):
    g = Grid(n)
    a = g.a
    n_rows, hd = o_ref.shape[3:]
    half = n_rows // 2
    lo, hi = pl.ds(0, half), pl.ds(half, half)
    g.greet()
    g.greeted()
    order = sorted(range(a - 1), key=lambda r: -min(r + 1, a - 1 - r)) + [a - 1]

    ml_cp = remote(ml_ref, ml0, send0.at[2 * a], recv0.at[2 * a], g.partner())
    ml_cp.start()
    core_a, core_b = {}, {}
    for r in order:
        hy, hx = g.y_at(r + 1), g.x_at(r + 1)
        core_a[r] = remote(o_ref.at[1 - g.c, hy, :, lo], r0.at[hy, :, lo], send0.at[r], recv0.at[r], g.partner())
        core_b[r] = remote(o_ref.at[1 - g.c, :, hx, hi], r0.at[:, hx, hi], send0.at[a + r], recv0.at[a + r], g.partner())
        core_a[r].start()
        core_b[r].start()
    ml_cp.wait_recv()
    own = pl.ds(pl.multiple_of(g.c * a * a, a * a), a * a)
    top, fs, total = merge([ml_ref[0, own, :], ml0[0, own, :]], [ml_ref[1, own, :], ml0[1, own, :]])
    for i, v in enumerate([top, total] + fs):
        rows[i] = v
    for i in range(a):
        for k, (da, db) in enumerate(((mla, mlb), (mla, mlb), (fa, fb), (fa, fb))):
            dst = pl.ds(k % 2 * a, a)
            da[i, dst, :] = rows[k, pl.ds(i * a, a), :]
            db[i, dst, :] = rows[k, pl.ds(i, a, stride=a), :]

    ring1 = []
    for r in order:
        hy, hx = g.y_at(r + 1), g.x_at(r + 1)
        core_a[r].wait_recv()
        ft = fa[hy].T[:half]
        for j in range(a):
            r0[hy, j, lo] = o_ref[g.c, hy, j, lo] * ft[:, j:j + 1] + r0[hy, j, lo] * ft[:, a + j:a + j + 1]
        if r < a - 1:
            ring1 += [
                remote(mla.at[hy], rmla.at[r], send1.at[0, r], recv1.at[0, r], g.y_peer(r + 1)),
                remote(r0.at[hy, :, lo], r1a.at[r], send1.at[1, r], recv1.at[1, r], g.y_peer(r + 1)),
            ]
            ring1[-2].start()
            ring1[-1].start()
        core_b[r].wait_recv()
        ft = fb[hx].T[half:]
        for j in range(a):
            r0[j, hx, hi] = o_ref[g.c, j, hx, hi] * ft[:, j:j + 1] + r0[j, hx, hi] * ft[:, a + j:a + j + 1]
        if r < a - 1:
            ring1 += [
                remote(mlb.at[hx], rmlb.at[r], send1.at[2, r], recv1.at[2, r], g.x_peer(r + 1)),
                remote(r0.at[:, hx, hi], r1b.at[r], send1.at[3, r], recv1.at[3, r], g.x_peer(r + 1)),
            ]
            ring1[-2].start()
            ring1[-1].start()
    for cp in ring1:
        cp.wait_recv()

    for side, (ml_own, ml_got, dst, sm) in enumerate(((mla, rmla, s2a, sm2a), (mlb, rmlb, s2b, sm2b))):
        place = g.x if side else g.y
        parts = [ml_own.at[place]] + [ml_got.at[r] for r in range(a - 1)]
        top, fs, total = merge([p[pl.ds(0, a), :] for p in parts], [p[pl.ds(a, a), :] for p in parts])
        for s in range(a):
            fcol[pl.ds(s * a, a), :] = fs[s]
        rows[0, pl.ds(0, a), :] = top
        rows[1, pl.ds(0, a), :] = total
        ft = fcol[...].T[half * side:half * (side + 1)]
        for j in range(a):
            sm[j, 0:1, :] = rows[0, j:j + 1, :]
            sm[j, 1:2, :] = rows[1, j:j + 1, :]
            acc = (r0[j, g.x, hi] if side else r0[g.y, j, lo]) * ft[:, j:j + 1]
            for r in range(a - 1):
                got = r1b[r, j] if side else r1a[r, j]
                acc = acc + got * ft[:, (r + 1) * a + j:(r + 1) * a + j + 1]
            dst[j] = acc

    ring2 = []
    for r in order[:-1]:
        hy, hx = g.y_at(r + 1), g.x_at(r + 1)
        ring2 += [
            remote(sm2a.at[hx], rm2a.at[r], send2.at[0, r], recv2.at[0, r], g.x_peer(r + 1)),
            remote(s2a.at[hx], r2a.at[r], send2.at[1, r], recv2.at[1, r], g.x_peer(r + 1)),
            remote(sm2b.at[hy], rm2b.at[r], send2.at[2, r], recv2.at[2, r], g.y_peer(r + 1)),
            remote(s2b.at[hy], r2b.at[r], send2.at[3, r], recv2.at[3, r], g.y_peer(r + 1)),
        ]
    for cp in ring2:
        cp.start()
    for cp in ring2:
        cp.wait_recv()
    for side, (sm, rm, mine, got) in enumerate(((sm2a, rm2a, s2a, r2a), (sm2b, rm2b, s2b, r2b))):
        place = g.y if side else g.x
        parts = [sm.at[place]] + [rm.at[r] for r in range(a - 1)]
        top, fs, total = merge([p[0:1, :] for p in parts], [p[1:2, :] for p in parts])
        for s in range(a):
            fcol[pl.ds(s, 1), :] = fs[s]
        fcol[pl.ds(a, 1), :] = total
        ft = fcol[...].T[half * side:half * (side + 1)]
        acc = mine[place] * ft[:, 0:1]
        for r in range(a - 1):
            acc = acc + got[r] * ft[:, r + 1:r + 2]
        go[g.c, (hi if side else lo), :] = (acc / ft[:, a:a + 1]).astype(BF16)

    heads = remote(go.at[g.c], go.at[g.c], osem.at[0], osem.at[1], g.partner())
    heads.start()
    heads.wait_recv()
    lhs = jnp.concatenate([go[0], go[1]], axis=1)
    for i in range(a):
        part = jnp.dot(lhs, wo_ref[:, pl.ds(i * a * hd, a * hd)], preferred_element_type=F32)
        for j in range(a):
            r0y[i, j] = part[:, j * hd:(j + 1) * hd]
    ring3, ring4 = [], []
    for r in order[:-1]:
        hy, hx = g.y_at(r + 1), g.x_at(r + 1)
        ring3 += [
            remote(r0y.at[hy, :, lo], y1a.at[r], send3.at[0, r], recv3.at[0, r], g.y_peer(r + 1)),
            remote(r0y.at[:, hx, hi], y1b.at[r], send3.at[1, r], recv3.at[1, r], g.x_peer(r + 1)),
        ]
    for cp in ring3:
        cp.start()
    for cp in ring3:
        cp.wait_recv()
    t2a[...] = functools.reduce(jnp.add, [y1a[r] for r in range(a - 1)], r0y[g.y, :, lo])
    t2b[...] = functools.reduce(jnp.add, [y1b[r] for r in range(a - 1)], r0y[:, g.x, hi])
    for r in order[:-1]:
        hy, hx = g.y_at(r + 1), g.x_at(r + 1)
        ring4 += [
            remote(t2a.at[hx], y2a.at[r], send4.at[0, r], recv4.at[0, r], g.x_peer(r + 1)),
            remote(t2b.at[hy], y2b.at[r], send4.at[1, r], recv4.at[1, r], g.y_peer(r + 1)),
        ]
    for cp in ring4:
        cp.start()
    for cp in ring4:
        cp.wait_recv()
    y_out[g.c, g.y, g.x, lo, :] = functools.reduce(jnp.add, [y2a[r] for r in range(a - 1)], t2a[g.x]).astype(BF16)
    y_out[g.c, g.y, g.x, hi, :] = functools.reduce(jnp.add, [y2b[r] for r in range(a - 1)], t2b[g.y]).astype(BF16)
    outs = Gather(g, y_out, bsend, brecv)
    outs.start()
    outs.finish()
    for cp in [ml_cp, heads] + list(core_a.values()) + list(core_b.values()) + ring1 + ring2 + ring3 + ring4:
        cp.wait_send()


def solution(mesh):
    n = mesh.shape['sp']
    a = math.isqrt(n // 2)
    vmem, hbm, smem = (pl.BlockSpec(memory_space=s) for s in (pltpu.VMEM, pltpu.HBM, pltpu.SMEM))
    dma = pltpu.SemaphoreType.DMA

    def stay(x):
        return pltpu.with_memory_space_constraint(x, pltpu.HBM)

    def local_step(tokens, w_query, w_key, w_value, w_out, k_cache, v_cache, positions):
        n_rows, t_loc, hd = k_cache.shape
        d_model = tokens.shape[1]
        half = n_rows // 2
        f32 = lambda *s: pltpu.VMEM(s, F32)
        bf16 = lambda *s: pltpu.VMEM(s, BF16)
        shape = jax.ShapeDtypeStruct
        blk = 16
        sems = [dma((Gather.sems(a),))] * 2
        cache = shape(k_cache.shape, k_cache.dtype)
        n_part = 4
        q_all, kv_new, wo, k_vm, v_vm = pl.pallas_call(
            functools.partial(project_kernel, n),
            out_shape=(shape((2, n // 2, n_rows, hd), BF16), shape((2, n_rows, hd), F32), shape((2 * w_out.shape[0], w_out.shape[1] // 2), BF16), cache, cache),
            in_specs=[hbm] * 7,
            out_specs=(vmem,) * 5,
            scratch_shapes=[bf16(n_rows, d_model), bf16(n_part, d_model, w_query.shape[1] // 2 // n_part), bf16(d_model, 2 * hd), dma((4,)), dma((n_part,)), dma((2,)), dma((4,))],
            compiler_params=pltpu.CompilerParams(collective_id=0, has_side_effects=True, vmem_limit_bytes=22 << 20),
            name='project',
        )(*map(stay, (tokens, w_query, w_key, w_value, w_out, k_cache, v_cache)))
        k_upd, v_upd, o, ml, _, _ = pl.pallas_call(
            functools.partial(attend_kernel, blk),
            out_shape=(cache, cache, shape((n * n_rows, hd), F32), shape((2, n, n_rows), F32), cache, cache),
            in_specs=[smem] + [vmem] * 4,
            out_specs=(hbm, hbm) + (vmem,) * 4,
            input_output_aliases={3: 4, 4: 5},
            scratch_shapes=[f32(n * n_rows, hd), f32(blk, n, t_loc), bf16(blk, n, t_loc)] + [dma((2, n_rows // blk))],
            compiler_params=pltpu.CompilerParams(vmem_limit_bytes=8 << 20),
            name='attend',
        )(positions, q_all.reshape(n, n_rows, hd), kv_new, k_vm, v_vm)
        y = pl.pallas_call(
            functools.partial(combine_kernel, n),
            out_shape=shape((2, a, a, n_rows, w_out.shape[1] // n), BF16),
            in_specs=[vmem] * 3,
            out_specs=vmem,
            scratch_shapes=[f32(a, a, n_rows, hd), f32(2, n, n_rows), f32(4, a * a, n_rows)]
            + [f32(a, 2 * a, n_rows)] * 2 + [f32(max(a * a, 8), n_rows)] + [f32(a, 2 * a, n_rows)] * 2
            + [f32(a - 1, a, half, hd)] * 2 + [f32(a - 1, 2 * a, n_rows)] * 2
            + [f32(a, half, hd)] * 2 + [f32(a, 8, n_rows)] * 2 + [f32(a - 1, half, hd)] * 2 + [f32(a - 1, 8, n_rows)] * 2
            + [bf16(2, n_rows, hd), f32(a, a, n_rows, hd)] + [f32(a - 1, a, half, hd)] * 2 + [f32(a, half, hd)] * 2 + [f32(a - 1, half, hd)] * 2
            + [dma((2 * a + 1,))] * 2 + [dma((4, a - 1))] * 4 + [dma((2,))] + [dma((2, a - 1))] * 4 + sems,
            compiler_params=pltpu.CompilerParams(collective_id=1, has_side_effects=True, vmem_limit_bytes=16 << 20),
            name='combine',
        )(o.reshape(2, a, a, n_rows, hd), ml, wo)
        y = y.reshape(n, n_rows, -1).transpose(1, 0, 2).reshape(n_rows, -1)
        return y, k_upd, v_upd

    cache_spec = P('dp', 'sp', None)
    return jax.shard_map(local_step, mesh=mesh, in_specs=(P('dp', None), P(), P(), P(), P('sp', None), cache_spec, cache_spec, P('dp')), out_specs=(P('dp', None), cache_spec, cache_spec), check_vma=False)
```

```python
import functools
import math

import jax
import jax.numpy as jnp
from jax import lax
from jax.experimental import pallas as pl
from jax.experimental.pallas import tpu as pltpu
from jax.sharding import PartitionSpec as P

MESH = pl.DeviceIdType.MESH
BF16, F32 = jnp.bfloat16, jnp.float32
LOWEST = -3.0e38


class Grid:
    def __init__(self, n):
        self.n = n
        self.a = a = math.isqrt(n // 2)
        me = lax.axis_index('sp')
        self.me = me
        self.c = lax.rem(me, 2)
        self.x = lax.rem(me // 2, a)
        self.y = me // (2 * a)

    def index(self, y, x, c):
        return (y * self.a + x) * 2 + c

    def y_at(self, r):
        return lax.rem(self.y + r, self.a)

    def x_at(self, r):
        return lax.rem(self.x + r, self.a)

    def y_peer(self, r):
        return self.index(self.y_at(r), self.x, self.c)

    def x_peer(self, r):
        return self.index(self.y, self.x_at(r), self.c)

    def partner(self):
        return self.index(self.y, self.x, 1 - self.c)

    def peers(self):
        out = [self.partner()]
        for r in range(1, self.a):
            out += [self.y_peer(r), self.x_peer(r)]
        return out

    def greet(self):
        barrier = pltpu.get_barrier_semaphore()
        for p in self.peers():
            pl.semaphore_signal(barrier, inc=1, device_id={'sp': p}, device_id_type=MESH)

    def greeted(self):
        pl.semaphore_wait(pltpu.get_barrier_semaphore(), 2 * self.a - 1)


def remote(src, dst, send, recv, dev):
    return pltpu.make_async_remote_copy(src_ref=src, dst_ref=dst, send_sem=send, recv_sem=recv, device_id={'sp': dev}, device_id_type=MESH)


class Gather:
    def __init__(self, g, buf, send, recv):
        self.g, self.buf, self.send, self.recv = g, buf, send, recv
        rows = buf.shape[3]
        self.half = (pl.ds(0, rows // 2), pl.ds(rows // 2, rows // 2))
        self.order = sorted(range(1, g.a), key=lambda r: -min(r, g.a - r))
        self.k = 0

    def cp(self, ref, dev):
        c = remote(ref, ref, self.send.at[self.k], self.recv.at[self.k], dev)
        self.k += 1
        c.start()
        return c

    def start(self):
        g, buf = self.g, self.buf
        self.first, self.late = {}, []
        for r in self.order:
            self.first[0, r] = self.cp(buf.at[g.c, g.y, g.x, self.half[0]], g.y_peer(r))
            self.first[1, r] = self.cp(buf.at[g.c, g.y, g.x, self.half[1]], g.x_peer(r))
        for r in self.order:
            self.late.append(((0, 0, r), self.cp(buf.at[g.c, g.y, g.x, self.half[0]], g.x_peer(r))))
            self.late.append(((1, 0, r), self.cp(buf.at[g.c, g.y, g.x, self.half[1]], g.y_peer(r))))
        self.core = [self.cp(buf.at[g.c, g.y, g.x], g.partner())]

    def finish(self):
        g, buf, a = self.g, self.buf, self.g.a
        for r in self.order[::-1]:
            for s in range(2):
                self.first[s, r].wait_recv()
                src = buf.at[g.c, g.y_at(a - r), g.x, self.half[0]] if s == 0 else buf.at[g.c, g.y, g.x_at(a - r), self.half[1]]
                for q in self.order:
                    self.late.append(((s, r, q), self.cp(src, g.x_peer(q) if s == 0 else g.y_peer(q))))
                self.core.append(self.cp(src, g.partner()))
        for (s, r, q), c in self.late:
            c.wait_recv()
            if s == 0:
                src = buf.at[g.c, g.y_at((a - r) % a), g.x_at(a - q), self.half[0]]
            else:
                src = buf.at[g.c, g.y_at(a - q), g.x_at((a - r) % a), self.half[1]]
            self.core.append(self.cp(src, g.partner()))
        for c in self.core:
            c.wait_recv()
        for c in list(self.first.values()) + [c for _, c in self.late] + self.core:
            c.wait_send()

    @staticmethod
    def sems(a):
        return 4 * (a - 1) + 1 + 2 * (a - 1) * a + 2 * (a - 1) * a


def project_kernel(n, x_hbm, wq_hbm, wk_hbm, wv_hbm, wo_hbm, k_hbm, v_hbm, q_out, kv_out, wo_out, k_out, v_out, xv, wqv, wkv, lsem, qsem, csem, rsem):
    g = Grid(n)
    hd = kv_out.shape[2]
    width = wq_hbm.shape[1] // 2
    n_part, part = wqv.shape[0], wqv.shape[2]
    x_cp = pltpu.make_async_copy(x_hbm, xv, lsem.at[0])
    q_cps = [
        pltpu.make_async_copy(wq_hbm.at[:, pl.ds(pl.multiple_of(g.c * width + i * part, part), part)], wqv.at[i], qsem.at[i])
        for i in range(n_part)
    ]
    kv_cps = [
        pltpu.make_async_copy(wk_hbm, wkv.at[:, pl.ds(0, hd)], lsem.at[1]),
        pltpu.make_async_copy(wv_hbm, wkv.at[:, pl.ds(hd, hd)], lsem.at[2]),
    ]
    rows, half = wo_hbm.shape[0], wo_hbm.shape[1] // 2
    mine = wo_out.at[pl.ds(pl.multiple_of(g.c * rows, rows), rows)]
    wo_cp = pltpu.make_async_copy(wo_hbm.at[:, pl.ds(pl.multiple_of(g.c * half, half), half)], mine, lsem.at[3])
    wo_swap = remote(wo_hbm.at[:, pl.ds(pl.multiple_of((1 - g.c) * half, half), half)], mine, rsem.at[0], rsem.at[1], g.partner())
    cache_cps = [pltpu.make_async_copy(k_hbm, k_out, csem.at[0]), pltpu.make_async_copy(v_hbm, v_out, csem.at[1])]
    x_cp.start()
    for cp in q_cps + kv_cps:
        cp.start()
    barrier = pltpu.get_barrier_semaphore()
    pl.semaphore_signal(barrier, inc=1, device_id={'sp': g.partner()}, device_id_type=MESH)
    x_cp.wait()
    per = part // hd
    first = g.c * (n // 4)
    for i in range(n_part):
        q_cps[i].wait()
        if i == n_part - 2:
            cache_cps[0].start()
        q = jnp.dot(xv[...], wqv[i], preferred_element_type=F32).astype(BF16)
        for j in range(i * per, (i + 1) * per):
            q_out[j % 2, first + j // 2] = q[:, (j - i * per) * hd:(j - i * per + 1) * hd]
    cache_cps[1].start()
    pl.semaphore_wait(barrier, 1)
    heads = q_out.at[:, pl.ds(first, n // 4)]
    q_swap = remote(heads, heads, rsem.at[2], rsem.at[3], g.partner())
    q_swap.start()
    wo_swap.start()
    wo_cp.start()
    for cp in kv_cps:
        cp.wait()
    kv = jnp.dot(xv[...], wkv[...], preferred_element_type=F32).astype(BF16)
    kv_out[0] = kv[:, :hd].astype(F32)
    kv_out[1] = kv[:, hd:].astype(F32)
    q_swap.wait()
    wo_swap.wait()
    for cp in [wo_cp] + cache_cps:
        cp.wait()


def attend_kernel(blk, pos, q_ref, kv_new, k_in, v_in, ko_hbm, vo_hbm, o_ref, ml_ref, kbuf, vbuf, q32, s_s, w_s, wsem):
    n_rows, t_loc, hd = kbuf.shape
    n_heads = o_ref.shape[0] // n_rows
    n_blk = n_rows // blk
    base = lax.axis_index('sp') * t_loc
    scale = hd ** -0.5 * math.log2(math.e)

    def writes(i):
        rows = pl.ds(i * blk, blk)
        return (pltpu.make_async_copy(kbuf.at[rows], ko_hbm.at[rows], wsem.at[0, i]), pltpu.make_async_copy(vbuf.at[rows], vo_hbm.at[rows], wsem.at[1, i]))

    @pl.loop(0, n_heads)
    def _(h):
        q32[pl.ds(h * n_rows, n_rows), :] = q_ref[h].astype(F32)

    ml_ref[...] = jnp.zeros_like(ml_ref)
    lane = lax.broadcasted_iota(jnp.int32, (n_heads, t_loc), 1)
    lane_b = lax.broadcasted_iota(jnp.int32, (n_heads, n_rows), 1)
    tile_row = lax.broadcasted_iota(jnp.int32, (16, hd), 0)

    def intake(i):
        stores = []
        for u in range(blk):
            b = i * blk + u
            p = pos[b] - base
            t0 = pl.multiple_of(jnp.clip(p, 0, t_loc - 1) // 16 * 16, 16)
            hit = tile_row == p - t0
            for which, buf in enumerate((kbuf, vbuf)):
                new = jnp.broadcast_to(kv_new[which, pl.ds(b, 1), :], (16, hd))
                old = buf[b, pl.ds(t0, 16), :].astype(F32)
                stores.append((buf, b, t0, jnp.where(hit, new, old).astype(BF16)))
        for buf, b, t0, v in stores:
            buf[b, pl.ds(t0, 16), :] = v
        for cp in writes(i):
            cp.start()

    def step(i, qk, soft, pv):
        outs, scores = [], []
        if pv:
            for u in range(blk):
                b = (i - 2) * blk + u
                outs.append((b, jnp.dot(w_s[u], vbuf[b], preferred_element_type=F32)))
        if soft:
            m_acc, l_acc = ml_ref[0], ml_ref[1]
            ss = [s_s[u] for u in range(blk)]
        if qk:
            for u in range(blk):
                b = i * blk + u
                qb = q32[pl.ds(b, n_heads, stride=n_rows), :].astype(BF16)
                scores.append(lax.dot_general(qb, kbuf[b], (((1,), (1,)), ((), ())), preferred_element_type=F32))
        if soft:
            for u, s in enumerate(ss):
                b = (i - 1) * blk + u
                s = jnp.where(lane <= pos[b] - base, s * scale, -jnp.inf)
                m = jnp.maximum(jnp.max(s, axis=1, keepdims=True), LOWEST)
                w = jnp.exp2(s - m)
                l = jnp.sum(w, axis=1, keepdims=True)
                w_s[u] = w.astype(BF16)
                m_acc = jnp.where(lane_b == b, m, m_acc)
                l_acc = jnp.where(lane_b == b, l, l_acc)
            ml_ref[0] = m_acc
            ml_ref[1] = l_acc
        for u, s in enumerate(scores):
            s_s[u] = s
        for b, o in outs:
            o_ref[pl.ds(b, n_heads, stride=n_rows), :] = o

    intake(0)
    step(0, True, False, False)
    intake(1)
    step(1, True, True, False)

    @pl.loop(2, n_blk)
    def _(i):
        intake(i)
        step(i, True, True, True)

    step(n_blk, False, True, True)
    step(n_blk + 1, False, False, True)

    @pl.loop(0, n_blk)
    def _(i):
        for cp in writes(i):
            cp.wait()


def merge(ms, ls):
    top = functools.reduce(jnp.maximum, ms)
    fs = [jnp.exp2(m - top) for m in ms]
    total = functools.reduce(jnp.add, [l * f for l, f in zip(ls, fs)])
    return top, fs, total


def combine_kernel(n, o_ref, ml_ref, wo_ref, y_out, r0, ml0, rows, fa, fb, fcol, mla, mlb, r1a, r1b, rmla, rmlb, s2a, s2b, sm2a, sm2b, r2a, r2b, rm2a, rm2b, go, r0y, y1a, y1b, t2a, t2b, y2a, y2b, send0, recv0, send1, recv1, send2, recv2, osem, send3, recv3, send4, recv4, bsend, brecv):
    g = Grid(n)
    a = g.a
    n_rows, hd = o_ref.shape[3:]
    half = n_rows // 2
    lo, hi = pl.ds(0, half), pl.ds(half, half)
    g.greet()
    g.greeted()
    order = sorted(range(1, a), key=lambda r: -min(r, a - r)) + [0]
    started = []

    def go_copy(src, dst, send, recv, dev):
        cp = remote(src, dst, send, recv, dev)
        cp.start()
        started.append(cp)
        return cp

    ml_cp = go_copy(ml_ref, ml0, send0.at[2 * a], recv0.at[2 * a], g.partner())
    core_a, core_b = {}, {}
    for r in order:
        hy, hx = g.y_at(r), g.x_at(r)
        core_a[r] = go_copy(o_ref.at[1 - g.c, hy, :, lo], r0.at[hy, :, lo], send0.at[r], recv0.at[r], g.partner())
        core_b[r] = go_copy(o_ref.at[1 - g.c, :, hx, hi], r0.at[:, hx, hi], send0.at[a + r], recv0.at[a + r], g.partner())
    ml_cp.wait_recv()
    own = pl.ds(pl.multiple_of(g.c * a * a, a * a), a * a)
    top, fs, total = merge([ml_ref[0, own, :], ml0[0, own, :]], [ml_ref[1, own, :], ml0[1, own, :]])
    for i, v in enumerate([top, total] + fs):
        rows[i] = v
    for i in range(a):
        for k, (da, db) in enumerate(((mla, mlb), (mla, mlb), (fa, fb), (fa, fb))):
            dst = pl.ds(k % 2 * a, a)
            da[i, dst, :] = rows[k, pl.ds(i * a, a), :]
            db[i, dst, :] = rows[k, pl.ds(i, a, stride=a), :]

    ml1, ring1 = {}, {}

    def send_heads(r, qs):
        hy, hx = g.y_at(r), g.x_at(r)
        for q in qs:
            ring1[0, r, q] = go_copy(r0.at[hy, g.x_at(q), lo], r1a.at[r - 1, q], send1.at[0, r, q], recv1.at[0, r, q], g.y_peer(r))
            ring1[1, r, q] = go_copy(r0.at[g.y_at(q), hx, hi], r1b.at[r - 1, q], send1.at[1, r, q], recv1.at[1, r, q], g.x_peer(r))

    for r in order:
        hy, hx = g.y_at(r), g.x_at(r)
        if r:
            ml1[0, r] = go_copy(mla.at[hy], rmla.at[r - 1], send1.at[2, r, 0], recv1.at[2, r, 0], g.y_peer(r))
            ml1[1, r] = go_copy(mlb.at[hx], rmlb.at[r - 1], send1.at[2, r, 1], recv1.at[2, r, 1], g.x_peer(r))
        core_a[r].wait_recv()
        ft = fa[hy].T[:half]
        for j in range(a):
            r0[hy, j, lo] = o_ref[g.c, hy, j, lo] * ft[:, j:j + 1] + r0[hy, j, lo] * ft[:, a + j:a + j + 1]
        core_b[r].wait_recv()
        ft = fb[hx].T[half:]
        for j in range(a):
            r0[j, hx, hi] = o_ref[g.c, j, hx, hi] * ft[:, j:j + 1] + r0[j, hx, hi] * ft[:, a + j:a + j + 1]
        if r:
            send_heads(r, order[:2])
    for r in order[:-1]:
        send_heads(r, order[2:])
    for cp in ml1.values():
        cp.wait_recv()

    ring2 = []
    for i, q in enumerate(order):
        hy, hx = g.y_at(q), g.x_at(q)
        for side, (ml_own, ml_got, dst, sm) in enumerate(((mla, rmla, s2a, sm2a), (mlb, rmlb, s2b, sm2b))):
            head = hy if side else hx
            parts = [ml_own.at[g.x if side else g.y]] + [ml_got.at[r - 1] for r in range(1, a)]
            top, fs, total = merge([p[pl.ds(head, 1), :] for p in parts], [p[pl.ds(a + head, 1), :] for p in parts])
            fc = fcol.at[2 * i + side]
            for s in range(a):
                fc[s:s + 1, :] = fs[s]
            sm[head, 0:1, :] = top
            sm[head, 1:2, :] = total
            ft = fc[...].T[half * side:half * (side + 1)]
            acc = (r0[head, g.x, hi] if side else r0[g.y, head, lo]) * ft[:, 0:1]
            for r in range(1, a):
                ring1[side, r, q].wait_recv()
            for r in range(1, a):
                acc = acc + (r1b if side else r1a)[r - 1, q] * ft[:, r:r + 1]
            dst[head] = acc
            if q:
                rm, r2 = (rm2b, r2b) if side else (rm2a, r2a)
                peer = g.y_peer(q) if side else g.x_peer(q)
                ring2.append(go_copy(sm.at[head], rm.at[q - 1], send2.at[2 * side, q], recv2.at[2 * side, q], peer))
                ring2.append(go_copy(dst.at[head], r2.at[q - 1], send2.at[2 * side + 1, q], recv2.at[2 * side + 1, q], peer))
    for cp in ring2:
        cp.wait_recv()
    for side, (sm, rm, mine, got) in enumerate(((sm2a, rm2a, s2a, r2a), (sm2b, rm2b, s2b, r2b))):
        place = g.y if side else g.x
        parts = [sm.at[place]] + [rm.at[r] for r in range(a - 1)]
        top, fs, total = merge([p[0:1, :] for p in parts], [p[1:2, :] for p in parts])
        fc = fcol.at[2 * a + side]
        for s in range(a):
            fc[s:s + 1, :] = fs[s]
        fc[a:a + 1, :] = total
        ft = fc[...].T[half * side:half * (side + 1)]
        acc = mine[place] * ft[:, 0:1]
        for r in range(a - 1):
            acc = acc + got[r] * ft[:, r + 1:r + 2]
        go[g.c, (hi if side else lo), :] = (acc / ft[:, a:a + 1]).astype(BF16)

    go_copy(go.at[g.c], go.at[g.c], osem.at[0], osem.at[1], g.partner()).wait_recv()
    lhs = jnp.concatenate([go[0], go[1]], axis=1)
    for i in range(a):
        part = jnp.dot(lhs, wo_ref[:, pl.ds(i * a * hd, a * hd)], preferred_element_type=F32)
        for j in range(a):
            r0y[i, j] = part[:, j * hd:(j + 1) * hd]
    ring3, ring4 = {}, []
    for q in order:
        for r in order[:-1]:
            hy, hx = g.y_at(r), g.x_at(r)
            ring3[0, r, q] = go_copy(r0y.at[hy, g.x_at(q), lo], y1a.at[r - 1, q], send3.at[0, r, q], recv3.at[0, r, q], g.y_peer(r))
            ring3[1, r, q] = go_copy(r0y.at[g.y_at(q), hx, hi], y1b.at[r - 1, q], send3.at[1, r, q], recv3.at[1, r, q], g.x_peer(r))
    for q in order:
        hy, hx = g.y_at(q), g.x_at(q)
        for side in range(2):
            for r in range(1, a):
                ring3[side, r, q].wait_recv()
            got = y1b if side else y1a
            mine = r0y[hy, g.x, hi] if side else r0y[g.y, hx, lo]
            dst = t2b.at[hy] if side else t2a.at[hx]
            dst[...] = functools.reduce(jnp.add, [got[r - 1, q] for r in range(1, a)], mine)
            if q:
                ring4.append(go_copy(dst, (y2b if side else y2a).at[q - 1], send4.at[side, q], recv4.at[side, q], g.y_peer(q) if side else g.x_peer(q)))
    for cp in ring4:
        cp.wait_recv()
    y_out[g.c, g.y, g.x, lo, :] = functools.reduce(jnp.add, [y2a[r] for r in range(a - 1)], t2a[g.x]).astype(BF16)
    y_out[g.c, g.y, g.x, hi, :] = functools.reduce(jnp.add, [y2b[r] for r in range(a - 1)], t2b[g.y]).astype(BF16)
    outs = Gather(g, y_out, bsend, brecv)
    outs.start()
    outs.finish()
    for cp in started:
        cp.wait_send()


def solution(mesh):
    n = mesh.shape['sp']
    a = math.isqrt(n // 2)
    vmem, hbm, smem = (pl.BlockSpec(memory_space=s) for s in (pltpu.VMEM, pltpu.HBM, pltpu.SMEM))
    dma = pltpu.SemaphoreType.DMA

    def stay(x):
        return pltpu.with_memory_space_constraint(x, pltpu.HBM)

    def local_step(tokens, w_query, w_key, w_value, w_out, k_cache, v_cache, positions):
        n_rows, t_loc, hd = k_cache.shape
        d_model = tokens.shape[1]
        half = n_rows // 2
        f32 = lambda *s: pltpu.VMEM(s, F32)
        bf16 = lambda *s: pltpu.VMEM(s, BF16)
        shape = jax.ShapeDtypeStruct
        blk = 16
        sems = [dma((Gather.sems(a),))] * 2
        cache = shape(k_cache.shape, k_cache.dtype)
        n_part = 4
        q_all, kv_new, wo, k_vm, v_vm = pl.pallas_call(
            functools.partial(project_kernel, n),
            out_shape=(shape((2, n // 2, n_rows, hd), BF16), shape((2, n_rows, hd), F32), shape((2 * w_out.shape[0], w_out.shape[1] // 2), BF16), cache, cache),
            in_specs=[hbm] * 7,
            out_specs=(vmem,) * 5,
            scratch_shapes=[bf16(n_rows, d_model), bf16(n_part, d_model, w_query.shape[1] // 2 // n_part), bf16(d_model, 2 * hd), dma((4,)), dma((n_part,)), dma((2,)), dma((4,))],
            compiler_params=pltpu.CompilerParams(collective_id=0, has_side_effects=True, vmem_limit_bytes=22 << 20),
            name='project',
        )(*map(stay, (tokens, w_query, w_key, w_value, w_out, k_cache, v_cache)))
        k_upd, v_upd, o, ml, _, _ = pl.pallas_call(
            functools.partial(attend_kernel, blk),
            out_shape=(cache, cache, shape((n * n_rows, hd), F32), shape((2, n, n_rows), F32), cache, cache),
            in_specs=[smem] + [vmem] * 4,
            out_specs=(hbm, hbm) + (vmem,) * 4,
            input_output_aliases={3: 4, 4: 5},
            scratch_shapes=[f32(n * n_rows, hd), f32(blk, n, t_loc), bf16(blk, n, t_loc)] + [dma((2, n_rows // blk))],
            compiler_params=pltpu.CompilerParams(vmem_limit_bytes=8 << 20),
            name='attend',
        )(positions, q_all.reshape(n, n_rows, hd), kv_new, k_vm, v_vm)
        y = pl.pallas_call(
            functools.partial(combine_kernel, n),
            out_shape=shape((2, a, a, n_rows, w_out.shape[1] // n), BF16),
            in_specs=[vmem] * 3,
            out_specs=vmem,
            scratch_shapes=[f32(a, a, n_rows, hd), f32(2, n, n_rows), f32(4, a * a, n_rows)]
            + [f32(a, 2 * a, n_rows)] * 2 + [f32(2 * a + 2, 8, n_rows)] + [f32(a, 2 * a, n_rows)] * 2
            + [f32(a - 1, a, half, hd)] * 2 + [f32(a - 1, 2 * a, n_rows)] * 2
            + [f32(a, half, hd)] * 2 + [f32(a, 8, n_rows)] * 2 + [f32(a - 1, half, hd)] * 2 + [f32(a - 1, 8, n_rows)] * 2
            + [bf16(2, n_rows, hd), f32(a, a, n_rows, hd)] + [f32(a - 1, a, half, hd)] * 2 + [f32(a, half, hd)] * 2 + [f32(a - 1, half, hd)] * 2
            + [dma((2 * a + 1,))] * 2 + [dma((3, a, a))] * 2 + [dma((4, a))] * 2 + [dma((2,))] + [dma((2, a, a))] * 2 + [dma((2, a))] * 2 + sems,
            compiler_params=pltpu.CompilerParams(collective_id=1, has_side_effects=True, vmem_limit_bytes=16 << 20),
            name='combine',
        )(o.reshape(2, a, a, n_rows, hd), ml, wo)
        y = y.reshape(n, n_rows, -1).transpose(1, 0, 2).reshape(n_rows, -1)
        return y, k_upd, v_upd

    cache_spec = P('dp', 'sp', None)
    return jax.shard_map(local_step, mesh=mesh, in_specs=(P('dp', None), P(), P(), P(), P('sp', None), cache_spec, cache_spec, P('dp')), out_specs=(P('dp', None), cache_spec, cache_spec), check_vma=False)
```
